1024 devices in a mesh: gx: 16 (over z_lo), gy: 8 (over z_hi, y), gz: 8 (over x, core).
Axes of the slice: x: 4, y: 4, z: 32 (z_hi: 2, z_lo: 16; z = z_hi * 16 + z_lo), core: 2. Of those that a mesh axis runs over, the one named last changes fastest.
Arguments:
- tokens: bfloat16 [1024, 4096], P(('gy', 'gz'), 'gx'), may hold values from -6 to 6
- expert_ids: int32 [1024, 2], P(('gy', 'gz')), may hold values from 0 to 7, all different within a row; in each aligned block of 16 rows (0 to 15, 16 to 31, ...) at most 8 rows name the same one
- gate_probs: float32 [1024, 2], P(('gy', 'gz')), may hold values from 0.2 to 1
- gate_weight: bfloat16 [8, 4096, 16384], P('gy', None, ('gz', 'gx')), may hold values from -0.09375 to 0.09375
- up_weight: bfloat16 [8, 4096, 16384], P('gy', None, ('gz', 'gx')), may hold values from -0.09375 to 0.09375
- down_weight: bfloat16 [8, 16384, 4096], P('gy', 'gz', 'gx'), may hold values from -0.046875 to 0.046875
Outputs:
- moe_output: bfloat16 [1024, 4096], P(('gy', 'gz'), 'gx')
The draws below stay inside these ranges and needn't reach their ends.
Inputs may be any that keep to these rules, and one draw needn't show every extreme that they name: `expert_ids`: A token's two ids differ. Within each aligned block of 16 tokens no expert is named more than 8 times, and in some blocks one expert is named exactly 8 times.
All inputs are finite; a program needn't handle non-finite values.
Results may differ from the reference program's by a relative error of at most 0.0049.
Values may be sent and summed in bfloat16 or wider, within the bound.
No kernel may reach another device: no remote copies, remote signals or barrier semaphores. Data moves between devices by JAX's collectives and lax.ppermute only.
A program may use at most 32 MiB of HBM per device.

```python
import math
import jax
import jax.numpy as jnp
import numpy as np
from jax import lax

D = 4096
FF = 16384
EXPERTS = 8
TOK_DEV = 16
CAP = 8
TOKENS = 1024
SLOTS = 512


def steps_of(key, extent, pieces, low, largest):
    loudness, own = 1.0, jax.random.fold_in(key, 6)
    for position, blocks in pieces:
        heights = jnp.exp(jax.random.uniform(jax.random.fold_in(own, position), (blocks,), jnp.float32, low / len(pieces), largest / len(pieces)))
        loudness = loudness * jnp.repeat(heights, extent[position] // blocks).reshape([-1 if axis == position else 1 for axis in range(len(extent))])
    return loudness


def deal_out(rng, own, number, rows, amount, top, limit, slope):
    sequence = jax.random.permutation(rng, amount)
    crowded, usual = load_shares(amount, rows * top, limit, slope, True), load_shares(amount, rows * top, limit, slope, False)
    places = jnp.arange(amount)

    def named(tallies, rotation):
        used = int((tallies > 0).sum())
        fixed = max(1, used // 4)
        shifted = fixed + (places - fixed + rotation * (used - fixed)) % max(1, amount - fixed)
        return jnp.zeros((amount,), jnp.int32).at[sequence[jnp.where(places < fixed, places, shifted)]].set(jnp.asarray(tallies, jnp.int32))

    tallies = jnp.where(number % 4 == 0, named(crowded, number // 4), named(usual, number - number // 4 - 1))
    mixed = jax.random.permutation(jax.random.fold_in(own, 3), amount)
    donor, sink = mixed[0:amount // 2 * 2:2], mixed[1:amount // 2 * 2:2]
    room = jnp.minimum(tallies[donor] - 1, limit - tallies[sink]) // 2
    room = jnp.where((donor == sequence[0]) | (sink == sequence[0]) | (tallies[sink] == 0), 0, jnp.maximum(room, 0))
    shifted = jax.random.randint(jax.random.fold_in(own, 4), (amount // 2,), 0, 1 << 20) % (room + 1)
    tallies = tallies.at[donor].add(-shifted).at[sink].add(shifted)
    members = jnp.searchsorted(jnp.cumsum(tallies), jnp.arange(rows * top), side="right").astype(jnp.int32)
    listing = members.reshape(top, rows).T
    listing = listing[jax.random.permutation(jax.random.fold_in(own, 1), rows)]
    rotation = jax.random.randint(jax.random.fold_in(own, 2), (rows, 1), 0, top)
    return jnp.take_along_axis(listing, (jnp.arange(top)[None, :] + rotation) % top, axis=1)


def load_shares(amount, total, bound, slope, full):
    weights = [(1 << 20) // math.isqrt(rank ** slope) + 1 for rank in range(1, amount + 1)]
    largest = bound if full else min(bound, max(-(-total // amount), total * weights[0] // sum(weights)))
    least = 1 if total - largest >= amount - 1 else 0
    holding, surplus = [largest] + [least] * (amount - 1), total - largest - least * (amount - 1)
    while surplus > 0:
        free = [i for i in range(1, amount) if holding[i] < largest] or [i for i in range(1, amount) if holding[i] < bound]
        pool, remaining = sum([weights[i] for i in free]), surplus
        for i in free:
            addition = min(bound - holding[i], max(1, remaining * weights[i] // pool), surplus)
            holding[i] = holding[i] + addition
            surplus = surplus - addition
    return np.array(holding)


def scatter_about(own_key, dims, spread, reach, pieces=(), kind=jnp.bfloat16):
    array = spread * jax.random.normal(own_key, dims, jnp.float32)
    if pieces:
        array = array * steps_of(own_key, dims, pieces, -0.22, 0.18)
    return jnp.clip(array, -reach, reach).astype(kind)


def setup_inputs(seed: int = 0) -> dict:
    seeds = jax.random.split(jax.random.key(seed), 7)
    tokens = scatter_about(seeds[0], (TOKENS, D), 1.0, 6.0, ((0, 64), (1, 16)))
    expert_ids_keys = jax.random.split(jax.random.fold_in(seeds[1], 1), TOKENS // TOK_DEV)
    expert_ids_turns = jax.random.permutation(jax.random.fold_in(seeds[1], 3), TOKENS // TOK_DEV)
    expert_ids = jax.vmap(lambda own, number: deal_out(jax.random.fold_in(seeds[1], 2), own, number, TOK_DEV, EXPERTS, 2, CAP, 2))(expert_ids_keys, expert_ids_turns).reshape((TOKENS, 2))
    gate_probs = jnp.clip(0.2 + 0.8 * jax.random.uniform(seeds[2], (TOKENS, 2), jnp.float32) ** steps_of(seeds[2], (TOKENS, 2), ((0, 64),), -0.2, 0.2), 0.2, 1.0)
    gate_weight = scatter_about(seeds[3], (EXPERTS, D, FF), D ** -0.5, 0.09375, ((0, 8), (2, 128)))
    up_weight = scatter_about(seeds[4], (EXPERTS, D, FF), D ** -0.5, 0.09375, ((0, 8), (2, 128)))
    down_weight = scatter_about(seeds[5], (EXPERTS, FF, D), FF ** -0.5, 0.046875, ((0, 8), (1, 8), (2, 16)))
    return dict(tokens=tokens, expert_ids=expert_ids, gate_probs=gate_probs, gate_weight=gate_weight, up_weight=up_weight, down_weight=down_weight)


def slot_numbers(expert_ids):
    grouped = expert_ids.reshape(-1, 2 * TOK_DEV)
    labels = jnp.arange(EXPERTS, dtype=jnp.int32)
    onehot = (grouped[:, :, None] == labels[None, None, :]).astype(jnp.int32)
    before = jnp.cumsum(onehot, axis=1) - onehot
    slot_index = jnp.sum(before * onehot, axis=2)
    return slot_index.reshape(-1, 2).astype(jnp.int32)


def reference(tokens, expert_ids, gate_probs, gate_weight, up_weight, down_weight):
    slot_index = slot_numbers(expert_ids)
    owner_row = (jnp.arange(TOKENS, dtype=jnp.int32) // TOK_DEV)[:, None]
    places = owner_row * CAP + slot_index
    columns = jnp.arange(SLOTS, dtype=jnp.int32)

    def one_expert(running, expert):
        chosen = expert_ids == expert
        matches = chosen[:, :, None] & (places[:, :, None] == columns[None, None, :])
        matches = matches.astype(jnp.float32)
        picker = jnp.sum(matches, axis=1)
        combine_table = jnp.sum(matches * gate_probs[:, :, None], axis=1)
        buffer = jnp.dot(picker.T.astype(jnp.bfloat16), tokens, preferred_element_type=jnp.float32).astype(jnp.bfloat16)
        gate_act = jnp.dot(buffer, gate_weight[expert], preferred_element_type=jnp.float32)
        up_act = jnp.dot(buffer, up_weight[expert], preferred_element_type=jnp.float32)
        hidden = (jax.nn.silu(gate_act) * up_act).astype(jnp.bfloat16)
        expert_out = jnp.dot(hidden, down_weight[expert], preferred_element_type=jnp.float32)
        added = jnp.dot(combine_table, expert_out, precision=lax.Precision.HIGHEST, preferred_element_type=jnp.float32)
        return running + added, None

    running, _ = lax.scan(one_expert, jnp.zeros((TOKENS, D), jnp.float32), jnp.arange(EXPERTS, dtype=jnp.int32))
    return running.astype(jnp.bfloat16)
```

```python
import jax
import jax.numpy as jnp
from jax import lax
from jax.sharding import Mesh, PartitionSpec as P


EXPERTS = 8
CAP = 8
BF = jnp.bfloat16
F32 = jnp.float32
AXES = ("gxh", "gxl", "zh", "y", "x", "c")
SIZES = (4, 4, 2, 4, 4, 2)


def sent_to_all(value, axis):
    count = lax.axis_size(axis)
    return lax.all_to_all(
        jnp.broadcast_to(value[None], (count, *value.shape)), axis, 0, 0, tiled=True
    )


def route_tables(expert_ids, gate_probs, experts, capacity):
    token_count = expert_ids.shape[0]
    flattened = expert_ids.reshape(token_count * 2)
    labels = jnp.arange(experts, dtype=jnp.int32)
    onehot = (flattened[:, None] == labels[None, :]).astype(jnp.int32)
    before = jnp.cumsum(onehot, axis=0) - onehot
    slot_index = jnp.sum(before * onehot, axis=1)
    places = flattened * capacity + slot_index
    columns = jnp.arange(experts * capacity, dtype=jnp.int32)
    matches = (places[:, None] == columns[None, :]).astype(F32)
    matches = matches.reshape(token_count, 2, experts * capacity)
    picker = jnp.sum(matches, axis=1)
    combine_table = jnp.sum(matches * gate_probs[:, :, None], axis=1)
    return (picker, combine_table)


def swiglu(rows, gate_weight, up_weight):
    gate = jnp.dot(rows, gate_weight, preferred_element_type=F32)
    up = jnp.dot(rows, up_weight, preferred_element_type=F32)
    return (jax.nn.silu(gate) * up).astype(BF)


def layer(tokens, expert_ids, gate_probs, gate_weight, up_weight, down_weight):
    near = lax.axis_index("gxl")
    gate_weight, up_weight, down_weight = gate_weight[0], up_weight[0], down_weight[0]
    width = tokens.shape[1]
    picker, combine_table = route_tables(expert_ids, gate_probs, EXPERTS, CAP)

    slots = jnp.einsum("tr,tf->rf", picker.astype(BF), tokens, preferred_element_type=F32)
    slots = slots.astype(BF).reshape(1, EXPERTS, CAP, width)
    outgoing = jnp.broadcast_to(slots, (4, EXPERTS, CAP, width)).reshape(-1, CAP, width)
    arrived = lax.all_to_all(outgoing, ("gxh", "zh", "y"), 0, 0, tiled=True)
    arrived = arrived.reshape(4, EXPERTS * CAP, width)

    joined = lax.all_gather(arrived, "gxl", axis=0, tiled=False)
    block = joined.transpose(2, 1, 0, 3).reshape(EXPERTS * CAP, 16 * width)

    block, down = lax.optimization_barrier((block, down_weight.reshape(4, 4, 128, width)))
    downs = []
    for shift in range(4):
        there = lax.bitwise_and(near + shift, 3)
        part = lax.dynamic_slice(down, (0, there, 0, 0), (4, 1, 128, width)).reshape(512, width)
        if shift:
            part = lax.ppermute(part, "gxl", [(i, (i + shift) % 4) for i in range(4)])
        downs.append(part)

    own = sent_to_all(block, "x").reshape(4 * EXPERTS * CAP, 16 * width)
    other = lax.ppermute(own, "c", [(0, 1), (1, 0)])

    hidden = jnp.concatenate(
        [swiglu(own, gate_weight, up_weight), swiglu(other, gate_weight, up_weight)], axis=0
    )
    hidden = lax.all_gather(hidden, "gxh", axis=1, tiled=True)

    half = hidden.shape[0] // 2
    parts_other = [jnp.dot(hidden[half:], w, preferred_element_type=F32).astype(BF) for w in downs]
    parts_own = [jnp.dot(hidden[:half], w, preferred_element_type=F32) for w in downs]
    received = lax.ppermute(jnp.stack(parts_other), "c", [(0, 1), (1, 0)])
    summed = jnp.stack(parts_own) + received.astype(F32)
    summed = summed.astype(BF).reshape(4, 4, EXPERTS * CAP, width).transpose(1, 0, 2, 3)
    summed = lax.all_to_all(summed, "x", 0, 0, tiled=True).astype(F32)
    place = jnp.arange(4, dtype=jnp.int32)
    order = (lax.bitwise_and(near - place[:, None], 3) == place[None, :]).astype(F32)
    placed = (order[:, None, :, None, None] * summed[None]).sum(axis=(1, 2))
    result = lax.all_to_all(placed.astype(BF), "gxl", 0, 0, tiled=True).astype(F32).sum(axis=0)

    result = result.astype(BF).reshape(EXPERTS, CAP, width)
    returned = lax.all_to_all(result, ("zh", "y"), 0, 0, tiled=True)
    table = returned.reshape(EXPERTS * CAP, width).astype(F32)
    out = jnp.dot(combine_table, table, precision=lax.Precision.HIGHEST, preferred_element_type=F32)
    return out.astype(BF)


def solution(mesh):
    split = Mesh(mesh.devices.reshape(SIZES), AXES)
    blocks, experts, hidden, features = ("zh", "y", "x", "c"), ("zh", "y"), ("x", "c"), ("gxh", "gxl")
    return jax.shard_map(
        layer,
        mesh=split,
        in_specs=(
            P(blocks, features),
            P(blocks, None),
            P(blocks, None),
            P(experts, None, hidden + features),
            P(experts, None, hidden + features),
            P(experts, hidden, features),
        ),
        out_specs=P(blocks, features),
        check_vma=False,
    )
```

```python
import jax
import jax.numpy as jnp
from jax import lax
from jax.experimental import pallas as pl
from jax.experimental.pallas import tpu as pltpu
from jax.sharding import Mesh, PartitionSpec as P


EXPERTS = 8
CAP = 8
BF = jnp.bfloat16
F32 = jnp.float32
AXES = ("gxh", "gxl", "zh", "y", "x", "c")
SIZES = (4, 4, 2, 4, 4, 2)


def sent_to_all(value, axis):
    count = lax.axis_size(axis)
    return lax.all_to_all(
        jnp.broadcast_to(value[None], (count, *value.shape)), axis, 0, 0, tiled=True
    )


def route_kernel(ids_ref, probs_ref, tokens_ref, slots_ref, table_ref):
    places, count = table_ref.shape
    row = lax.broadcasted_iota(jnp.int32, (places, count), 0)
    expert, slot = row // CAP, row % CAP
    first = expert == ids_ref[0:1, :]
    second = expert == ids_ref[1:2, :]
    named = first.astype(F32) + second.astype(F32)
    earlier = lax.broadcasted_iota(jnp.int32, (count, count), 0) < lax.broadcasted_iota(
        jnp.int32, (count, count), 1
    )
    before = jnp.dot(named.astype(BF), earlier.astype(F32).astype(BF), preferred_element_type=F32)
    at = slot.astype(F32)
    first = (first & (before == at)).astype(F32)
    second = (second & (before == at)).astype(F32)
    table_ref[...] = first * probs_ref[0:1, :] + second * probs_ref[1:2, :]
    picker = (first + second).astype(BF)
    rows = jnp.dot(picker, tokens_ref[...], preferred_element_type=F32).astype(BF)
    for copy in range(slots_ref.shape[0]):
        slots_ref[copy] = rows


def route(expert_ids, gate_probs, tokens, copies):
    count, width = tokens.shape
    return pl.pallas_call(
        route_kernel,
        out_shape=(
            jax.ShapeDtypeStruct((copies, EXPERTS * CAP, width), BF),
            jax.ShapeDtypeStruct((EXPERTS * CAP, count), F32),
        ),
        name="route",
    )(expert_ids.T, gate_probs.T, tokens)


def down_kernel(near_ref, hidden_ref, w0, w1, w2, w3, out_ref):
    hidden = hidden_ref[...]
    for shift, weight in enumerate((w0, w1, w2, w3)):
        part = jnp.dot(hidden, weight[...], preferred_element_type=F32)
        out_ref[lax.bitwise_and(near_ref[0] - shift, 3)] = part.astype(out_ref.dtype)


def down_projection(near, hidden, half, downs, dtype):
    rows, depth = hidden.shape[0] // 2, hidden.shape[1]
    width = downs[0].shape[1]
    whole = pl.BlockSpec((depth, width), lambda i, near: (0, 0))
    return pl.pallas_call(
        down_kernel,
        grid_spec=pltpu.PrefetchScalarGridSpec(
            num_scalar_prefetch=1,
            grid=(1,),
            in_specs=[pl.BlockSpec((rows, depth), lambda i, near: (half, 0))] + [whole] * 4,
            out_specs=pl.BlockSpec((4, rows, width), lambda i, near: (0, 0, 0)),
        ),
        out_shape=jax.ShapeDtypeStruct((4, rows, width), dtype),
        name="down",
    )(near, hidden, *downs)


def swiglu(rows, gate_weight, up_weight):
    gate = jnp.dot(rows, gate_weight, preferred_element_type=F32)
    up = jnp.dot(rows, up_weight, preferred_element_type=F32)
    return (jax.nn.silu(gate) * up).astype(BF)


def layer(tokens, expert_ids, gate_probs, gate_weight, up_weight, down_weight):
    near = lax.axis_index("gxl")
    gate_weight, up_weight, down_weight = gate_weight[0], up_weight[0], down_weight[0]
    width = tokens.shape[1]

    outgoing, combine_table = route(expert_ids, gate_probs, tokens, 4)
    outgoing = outgoing.reshape(-1, CAP, width)
    arrived = lax.all_to_all(outgoing, ("gxh", "zh", "y"), 0, 0, tiled=True)
    arrived = arrived.reshape(4, EXPERTS * CAP, width)

    joined = lax.all_gather(arrived, "gxl", axis=0, tiled=False)
    block = joined.transpose(2, 1, 0, 3).reshape(EXPERTS * CAP, 16 * width)

    block, down = lax.optimization_barrier((block, down_weight.reshape(4, 4, 128, width)))
    downs = []
    for shift in range(4):
        there = lax.bitwise_and(near + shift, 3)
        part = lax.dynamic_slice(down, (0, there, 0, 0), (4, 1, 128, width)).reshape(512, width)
        if shift:
            part = lax.ppermute(part, "gxl", [(i, (i + shift) % 4) for i in range(4)])
        downs.append(part)

    own = sent_to_all(block, "x").reshape(4 * EXPERTS * CAP, 16 * width)
    other = lax.ppermute(own, "c", [(0, 1), (1, 0)])

    hidden = jnp.concatenate(
        [swiglu(own, gate_weight, up_weight), swiglu(other, gate_weight, up_weight)], axis=0
    )
    hidden = lax.all_gather(hidden, "gxh", axis=1, tiled=True)

    place = near.reshape(1)
    for_other = down_projection(place, hidden, 1, downs, BF)
    summed = down_projection(place, hidden, 0, downs, F32)
    received = lax.ppermute(for_other, "c", [(0, 1), (1, 0)])
    summed = (summed + received.astype(F32)).astype(BF)
    summed = summed.reshape(16, EXPERTS * CAP, width)
    summed = lax.all_to_all(summed, ("gxl", "x"), 0, 0, tiled=True)
    result = summed.astype(F32).sum(axis=0)

    result = result.astype(BF).reshape(EXPERTS, CAP, width)
    returned = lax.all_to_all(result, ("zh", "y"), 0, 0, tiled=True)
    table = returned.reshape(EXPERTS * CAP, width).astype(F32)
    out = jnp.einsum(
        "rt,rf->tf",
        combine_table,
        table,
        precision=lax.Precision.HIGHEST,
        preferred_element_type=F32,
    )
    return out.astype(BF)


def solution(mesh):
    split = Mesh(mesh.devices.reshape(SIZES), AXES)
    blocks, experts, hidden, features = ("zh", "y", "x", "c"), ("zh", "y"), ("x", "c"), ("gxh", "gxl")
    return jax.shard_map(
        layer,
        mesh=split,
        in_specs=(
            P(blocks, features),
            P(blocks, None),
            P(blocks, None),
            P(experts, None, hidden + features),
            P(experts, None, hidden + features),
            P(experts, hidden, features),
        ),
        out_specs=P(blocks, features),
        check_vma=False,
    )
```

```python
import jax
import jax.numpy as jnp
from jax import lax
from jax.experimental import pallas as pl
from jax.sharding import Mesh, PartitionSpec as P


EXPERTS = 8
CAP = 8
BF = jnp.bfloat16
F32 = jnp.float32
AXES = ("gxh", "gxl", "zh", "y", "x", "c")
SIZES = (4, 4, 2, 4, 4, 2)


def sent_to_all(value, axis):
    count = lax.axis_size(axis)
    return lax.all_to_all(
        jnp.broadcast_to(value[None], (count, *value.shape)), axis, 0, 0, tiled=True
    )


def route_kernel(ids_ref, probs_ref, tokens_ref, slots_ref, table_ref):
    places, count = table_ref.shape
    row = lax.broadcasted_iota(jnp.int32, (places, count), 0)
    expert, slot = row // CAP, row % CAP
    first = expert == ids_ref[0:1, :]
    second = expert == ids_ref[1:2, :]
    named = first.astype(F32) + second.astype(F32)
    earlier = lax.broadcasted_iota(jnp.int32, (count, count), 0) < lax.broadcasted_iota(
        jnp.int32, (count, count), 1
    )
    before = jnp.dot(named.astype(BF), earlier.astype(F32).astype(BF), preferred_element_type=F32)
    at = slot.astype(F32)
    first = (first & (before == at)).astype(F32)
    second = (second & (before == at)).astype(F32)
    table_ref[...] = first * probs_ref[0:1, :] + second * probs_ref[1:2, :]
    picker = (first + second).astype(BF)
    rows = jnp.dot(picker, tokens_ref[...], preferred_element_type=F32).astype(BF)
    for copy in range(slots_ref.shape[0]):
        slots_ref[copy] = rows


def route(expert_ids, gate_probs, tokens, copies):
    count, width = tokens.shape
    return pl.pallas_call(
        route_kernel,
        out_shape=(
            jax.ShapeDtypeStruct((copies, EXPERTS * CAP, width), BF),
            jax.ShapeDtypeStruct((EXPERTS * CAP, count), F32),
        ),
        name="route",
    )(expert_ids.T, gate_probs.T, tokens)


def swiglu(rows, gate_weight, up_weight):
    gate = jnp.dot(rows, gate_weight, preferred_element_type=F32)
    up = jnp.dot(rows, up_weight, preferred_element_type=F32)
    return (jax.nn.silu(gate) * up).astype(BF)


def layer(tokens, expert_ids, gate_probs, gate_weight, up_weight, down_weight):
    near = lax.axis_index("gxl")
    gate_weight, up_weight, down_weight = gate_weight[0], up_weight[0], down_weight[0]
    width = tokens.shape[1]

    outgoing, combine_table = route(expert_ids, gate_probs, tokens, 4)
    outgoing = outgoing.reshape(-1, CAP, width)
    arrived = lax.all_to_all(outgoing, ("gxh", "zh", "y"), 0, 0, tiled=True)
    arrived = arrived.reshape(4, EXPERTS * CAP, width)

    joined = lax.all_gather(arrived, "gxl", axis=0, tiled=False)
    block = joined.transpose(2, 1, 0, 3).reshape(EXPERTS * CAP, 16 * width)

    down = down_weight.reshape(4, 4, 128, width)
    downs = []
    for shift in range(4):
        there = lax.bitwise_and(near + shift, 3)
        part = lax.dynamic_slice(down, (0, there, 0, 0), (4, 1, 128, width)).reshape(512, width)
        if shift:
            part = lax.ppermute(part, "gxl", [(i, (i + shift) % 4) for i in range(4)])
        downs.append(part)

    own = sent_to_all(block, "x").reshape(4 * EXPERTS * CAP, 16 * width)
    other = lax.ppermute(own, "c", [(0, 1), (1, 0)])

    hidden = jnp.concatenate(
        [swiglu(own, gate_weight, up_weight), swiglu(other, gate_weight, up_weight)], axis=0
    )
    hidden = lax.all_gather(hidden, "gxh", axis=0, tiled=False, axis_index_groups=[[0, 2, 3, 1]])
    hidden = jnp.concatenate([hidden[j] for j in (0, 3, 1, 2)], axis=1)

    half = hidden.shape[0] // 2
    hidden, downs = lax.optimization_barrier((hidden, downs))
    downs = lax.optimization_barrier(jnp.stack(downs))
    downs = [downs[shift] for shift in range(4)]
    for_other = [jnp.dot(hidden[half:], w, preferred_element_type=F32) for w in downs]
    own = [jnp.dot(hidden[:half], w, preferred_element_type=F32) for w in downs]
    received = lax.ppermute(jnp.stack(for_other).astype(BF), "c", [(0, 1), (1, 0)])
    place = jnp.arange(4, dtype=jnp.int32)
    order = (lax.bitwise_and(near - place[:, None], 3) == place[None, :]).astype(F32)
    summed = jnp.stack(own) + received.astype(F32)
    summed = (order[:, :, None, None] * summed[None]).sum(axis=1).astype(BF)
    summed = summed.reshape(4, 4, 2, 4, CAP, width).transpose(0, 3, 1, 2, 4, 5)
    summed = summed.reshape(64, 2 * CAP, width)
    summed = lax.all_to_all(summed, ("gxl", "y", "x"), 0, 0, tiled=True)
    summed = summed.reshape(4, 4, 4, 2, CAP, width).astype(F32).sum(axis=(0, 2))

    upper = lax.axis_index("zh") == 1
    lows, highs = summed[:, 0], summed[:, 1]
    kept = jnp.where(upper, highs, lows).reshape(4 * CAP, width)
    sent = jnp.where(upper, lows, highs).astype(BF).reshape(4 * CAP, width)
    got = lax.ppermute(sent, "zh", [(0, 1), (1, 0)]).astype(F32)
    low_table, high_table = combine_table[: 4 * CAP], combine_table[4 * CAP :]
    here = jnp.where(upper, high_table, low_table)
    there = jnp.where(upper, low_table, high_table)

    def mixed(table, values):
        return jnp.einsum(
            "rt,rf->tf",
            table,
            values,
            precision=lax.Precision.HIGHEST,
            preferred_element_type=F32,
        )

    out = mixed(here, kept) + mixed(there, got)
    return out.astype(BF)


def solution(mesh):
    split = Mesh(mesh.devices.reshape(SIZES), AXES)
    blocks, experts, hidden, features = ("zh", "y", "x", "c"), ("zh", "y"), ("x", "c"), ("gxh", "gxl")
    return jax.shard_map(
        layer,
        mesh=split,
        in_specs=(
            P(blocks, features),
            P(blocks, None),
            P(blocks, None),
            P(experts, None, hidden + features),
            P(experts, None, hidden + features),
            P(experts, hidden, features),
        ),
        out_specs=P(blocks, features),
        check_vma=False,
    )
```
